256 devices in a mesh: asset: 32 (over x, z), tm: 8 (over y, core).
Axes of the slice: x: 4, y: 4, z: 8, core: 2. Of those that a mesh axis runs over, the one named last changes fastest.
Arguments:
- prices: float32 [480, 61440], P('tm', 'asset'), may hold values from -10 to 20
- sectors: int32 [61440], P('asset'), may hold values from 0 to 10, as said below
- wanted: int32 [32, 8, 32], replicated, may hold values from -1 to 14, as said below
- pair_slots: int32 [32768, 2], P(('asset', 'tm')), may hold values from 0 to 31, as said below
- pair_count: int32 [256], P(('asset', 'tm')), may hold values from 16 to 128, as said below
Outputs:
- comovement: float32 [32768, 4, 2, 128], P(('asset', 'tm'))
The draws below stay inside these ranges and needn't reach their ends.
Inputs may be any that keep to these rules, and one draw needn't show every extreme that they name: Every one of the 11 sectors holds at least one series. `wanted`: every device needs a block from at least one column; in every draw some device needs one from every column. `pair_slots`: both columns of a pair row of device g = d * 8 + t have wanted[d, t, column] >= 0. `pair_count`: the rows in use are a device's first ones; some device uses all 128.
All inputs are finite; a program needn't handle non-finite values.
Results may differ from the reference program's by a relative error of at most 0.00046.
Values may be sent and summed in bfloat16 or wider, within the bound.
A program may use at most 128 MiB of HBM per device.

```python
import jax
import jax.numpy as jnp
from jax import lax

BLK = 128
SECT = 11
BLK_DEV = 15
PAIRS = 128
SERIES = 61440
TIME = 480
HOP = 30
WIN = 390
N_ASSET = 32
N_TM = 8


def sector_ids(key):
    folded = jax.random.fold_in(key, 11)
    drawn = jax.random.randint(folded, (SERIES,), 0, SECT)
    position = jnp.arange(SERIES, dtype=jnp.int32)
    return jnp.where(position < SECT, position, drawn).astype(jnp.int32)


def wanted_table(key):
    folded = jax.random.fold_in(key, 31)
    key_needed, key_forced, key_chosen, key_blocks = jax.random.split(folded, 4)
    needed = jax.random.randint(key_needed, (N_ASSET, N_TM, N_ASSET), 0, 2)
    forced = jax.random.randint(key_forced, (N_ASSET, N_TM), 0, N_ASSET)
    column = jnp.arange(N_ASSET, dtype=jnp.int32)
    needed = jnp.where(column[None, None, :] == forced[:, :, None], 1, needed)
    chosen = jax.random.randint(key_chosen, (), 0, N_ASSET * N_TM)
    position = jnp.arange(N_ASSET, dtype=jnp.int32)[:, None] * N_TM + jnp.arange(N_TM, dtype=jnp.int32)[None, :]
    needed = jnp.where((position == chosen)[:, :, None], 1, needed)
    blocks = jax.random.randint(key_blocks, (N_ASSET, N_TM, N_ASSET), 0, BLK_DEV)
    return jnp.where(needed > 0, blocks, -1).astype(jnp.int32)


def draw_sectors(key, part):
    return sector_ids(key)


def draw_prices(key, part):
    sector = sector_ids(key)
    subkeys = jax.random.split(jax.random.fold_in(key, 12), 4)
    onehot = (sector[:, None] == jnp.arange(SECT, dtype=jnp.int32)[None, :]).astype(jnp.float32)
    common = jax.random.normal(subkeys[0], (TIME, SECT), jnp.float32)
    specific = jax.random.normal(subkeys[1], (TIME, SERIES), jnp.float32)
    loading = jax.random.uniform(subkeys[2], (SERIES,), jnp.float32, 0.5, 1.5)
    growth = 1.0 + 2.0 * jnp.arange(SERIES, dtype=jnp.float32) / SERIES
    changes = growth * (loading * jnp.dot(common, onehot.T) + specific)
    opening = jax.random.uniform(subkeys[3], (SERIES,), jnp.float32, 3.0, 6.0)
    return opening + 0.01 * jnp.cumsum(changes, axis=0)


def draw_wanted(key, part):
    return wanted_table(key)


def draw_pair_slots(key, part):
    request_table = wanted_table(key).reshape(N_ASSET * N_TM, N_ASSET)
    filled = request_table >= 0
    filled_count = jnp.sum(filled.astype(jnp.int32), axis=1)
    column = jnp.arange(N_ASSET, dtype=jnp.int32)
    ordering = jnp.argsort(jnp.where(filled, 0, N_ASSET) + column[None, :], axis=1).astype(jnp.int32)
    random_picks = jax.random.randint(jax.random.fold_in(key, 32), (N_ASSET * N_TM, PAIRS * 2), 0, 1 << 20)
    rank_within = random_picks % filled_count[:, None]
    chosen = jnp.take_along_axis(ordering, rank_within, axis=1)
    return chosen.reshape(N_ASSET * N_TM * PAIRS, 2).astype(jnp.int32)


def draw_pair_count(key, part):
    folded = jax.random.fold_in(key, 41)
    key_counts, key_busiest = jax.random.split(folded)
    counts = jax.random.randint(key_counts, (N_ASSET * N_TM,), PAIRS // 8, PAIRS + 1)
    busiest = jax.random.randint(key_busiest, (), 0, N_ASSET * N_TM)
    return jnp.where(jnp.arange(N_ASSET * N_TM, dtype=jnp.int32) == busiest, PAIRS, counts).astype(jnp.int32)


def setup_inputs(seed: int = 0) -> dict:
    key_list = jax.random.split(jax.random.key(seed), 6)
    return {
        "prices": draw_prices(jax.random.fold_in(key_list[5], 71), 0),
        "sectors": draw_sectors(jax.random.fold_in(key_list[5], 71), 0),
        "wanted": draw_wanted(jax.random.fold_in(key_list[5], 71), 0),
        "pair_slots": draw_pair_slots(jax.random.fold_in(key_list[5], 71), 0),
        "pair_count": draw_pair_count(jax.random.fold_in(key_list[5], 71), 0),
    }


epsilon = 1e-06
highest = lax.Precision.HIGHEST

def moments(held, opening, closing):
    portion = held[opening:closing].astype(jnp.float32)
    average = lax.optimization_barrier(jnp.sum(portion, axis=0)) / (closing - opening)
    second = lax.optimization_barrier(jnp.sum(portion * portion, axis=0)) / (closing - opening)
    return (average, lax.rsqrt(second - average * average + epsilon))

def reference(prices, sectors, wanted, pair_slots, pair_count):
    earlier = jnp.concatenate([prices[:1], prices[:-1]], axis=0)
    returns = prices - earlier
    labels = jnp.arange(SECT, dtype=jnp.int32)
    member = (sectors[:, None] == labels[None, :]).astype(jnp.float32)
    totals = jnp.dot(returns, member, precision=highest)
    sector_mean = totals / lax.optimization_barrier(jnp.sum(member, axis=0))
    neutral = (returns - jnp.dot(sector_mean, member.T, precision=highest)).astype(jnp.bfloat16)
    blocks = neutral.reshape(TIME, N_ASSET, BLK_DEV, BLK)
    column_ids = jnp.arange(N_ASSET, dtype=jnp.int32)
    slot_rows = pair_slots.reshape(N_ASSET * N_TM, PAIRS, 2)
    request_rows = wanted.reshape(N_ASSET * N_TM, N_ASSET)
    edges = [0, HOP, 2 * HOP, 3 * HOP, WIN, WIN + HOP, WIN + 2 * HOP, TIME]

    def device(number):
        requests = request_rows[number]
        held = blocks[:, column_ids, jnp.maximum(requests, 0), :]
        held = jnp.where((requests >= 0)[None, :, None], held, jnp.zeros((), jnp.bfloat16))
        stats = [moments(held, window * HOP, window * HOP + WIN) for window in range(4)]
        center = jnp.stack([entry[0] for entry in stats], axis=1)
        inverse = jnp.stack([entry[1] for entry in stats], axis=1)
        chosen = slot_rows[number]
        first_block = held[:, chosen[:, 0], :].astype(jnp.float32)
        second_block = held[:, chosen[:, 1], :].astype(jnp.float32)
        pieces = [jnp.einsum('tpi,tpj->pij', first_block[edges[segment]:edges[segment + 1]], second_block[edges[segment]:edges[segment + 1]], precision=highest) for segment in range(7)]
        windows = [pieces[window] + pieces[window + 1] + pieces[window + 2] + pieces[window + 3] for window in range(4)]
        gram = jnp.stack(windows, axis=1)
        center_first = center[chosen[:, 0]]
        center_second = center[chosen[:, 1]]
        inverse_first = inverse[chosen[:, 0]]
        inverse_second = inverse[chosen[:, 1]]
        correlation = gram / WIN - center_first[..., :, None] * center_second[..., None, :]
        correlation = correlation * inverse_first[..., :, None] * inverse_second[..., None, :]
        square = WIN * correlation * correlation
        summary = jnp.stack([lax.optimization_barrier(jnp.mean(square, axis=3)), lax.optimization_barrier(jnp.mean(square, axis=2))], axis=2)
        in_use = jnp.arange(PAIRS, dtype=jnp.int32) < pair_count[number]
        return jnp.where(in_use[:, None, None, None], summary, jnp.zeros((), jnp.float32))
    summaries = lax.map(device, jnp.arange(N_ASSET * N_TM, dtype=jnp.int32))
    return summaries.reshape(N_ASSET * N_TM * PAIRS, 4, 2, BLK)
```

```python
import functools

import jax
import jax.numpy as jnp
from jax import lax
from jax.experimental import pallas as pl
from jax.experimental.pallas import tpu as pltpu
from jax.sharding import PartitionSpec as P

BLK = 128
SECT = 11
NX, NZ, NY, NC = 4, 8, 4, 2
NA, NT = NX * NZ, NY * NC
ROWS = 64
MINUTES = 60
HALF = 30
WIN = 390
NW = 4
MESH = pl.DeviceIdType.MESH

epsilon = 1e-06
highest = lax.Precision.HIGHEST


def shifted(block, axis, distance):
    devices = range(lax.axis_size(axis))
    route = [(i - distance, i) for i in devices if i - distance in devices]
    return lax.ppermute(block, axis, route)


def total_kernel(message, total, slots, send_sem, recv_sem):
    d = lax.axis_index("asset")
    t = lax.axis_index("tm")
    barrier = pltpu.get_barrier_semaphore()
    for k in range(1, NA):
        pl.semaphore_signal(barrier, inc=1, device_id=((d + k) % NA, t), device_id_type=MESH)
    pl.semaphore_wait(barrier, NA - 1)
    copies = []
    for k in range(1, NA):
        copy = pltpu.make_async_remote_copy(
            src_ref=message,
            dst_ref=slots.at[k],
            send_sem=send_sem.at[k],
            recv_sem=recv_sem.at[k],
            device_id=((d + k) % NA, t),
            device_id_type=MESH,
        )
        copy.start()
        copies.append(copy)
    subtotal = message[...]
    for k, copy in enumerate(copies):
        copy.wait_recv()
        subtotal = subtotal + slots[k + 1]
    total[...] = subtotal
    for copy in copies:
        copy.wait_send()


def summed(message):
    return pl.pallas_call(
        total_kernel,
        out_shape=jax.ShapeDtypeStruct(message.shape, message.dtype),
        in_specs=[pl.BlockSpec(memory_space=pltpu.VMEM)],
        out_specs=pl.BlockSpec(memory_space=pltpu.VMEM),
        scratch_shapes=[
            pltpu.VMEM((NA, *message.shape), message.dtype),
            pltpu.SemaphoreType.DMA((NA,)),
            pltpu.SemaphoreType.DMA((NA,)),
        ],
        compiler_params=pltpu.CompilerParams(collective_id=0, has_side_effects=True),
    )(message)


ORDER = (0, 1, 7, 2, 6, 3, 5, 4)
FIRST_HALF = 8


def exchange_kernel(
    requests, blocks, out, g1, g2, g3, g4, g5, g6, g7, picked, relay,
    z_send, z_recv, x_send, x_recv, y_send, y_recv, own_sem,
):
    d = lax.axis_index("asset")
    t = lax.axis_index("tm")
    x, z, y, c = d // NZ, d % NZ, t // NC, t % NC
    gathered = (blocks, g1, g2, g3, g4, g5, g6, g7)
    count = blocks.shape[0]

    def at_x(k):
        return ((x + k) % NX) * NZ + z, t

    def at_z(k):
        return x * NZ + (z + k + NZ) % NZ, t

    others = [(dy, dc) for dy in (1, 3, 2, 0) for dc in (0, 1) if (dy, dc) != (0, 0)]

    def at_y(k, sign):
        dy, dc = others[k]
        return d, ((y + sign * dy + NY) % NY) * NC + (c + dc) % NC

    barrier = pltpu.get_barrier_semaphore()
    peers = [at_z(1), at_z(-1)] + [at_x(k) for k in range(1, NX)]
    peers += [at_y(k, 1) for k in range(len(others))]
    for peer in peers:
        pl.semaphore_signal(barrier, inc=1, device_id=peer, device_id_type=MESH)

    pending = []

    def along_z(source, target, number, first, size, step):
        copy = pltpu.make_async_remote_copy(
            src_ref=gathered[source].at[pl.ds(first, size)],
            dst_ref=gathered[target].at[pl.ds(first, size)],
            send_sem=z_send.at[number],
            recv_sem=z_recv.at[number],
            device_id=at_z(step),
            device_id_type=MESH,
        )
        copy.start()
        pending.append(copy)
        return copy

    def pick(j):
        for k in (1, 3, 2, 0):
            def one(i, _):
                block = gathered[j][requests[(j * NX + k) * NT + i]]
                if k == 0:
                    relay[j, i, 0] = block
                else:
                    picked[j, k - 1, i] = block
                return 0
            lax.fori_loop(0, NT, one, 0)

    def along_x(j):
        copies = []
        for k in (1, 3, 2):
            copy = pltpu.make_async_remote_copy(
                src_ref=picked.at[j, k - 1],
                dst_ref=relay.at[j, :, k],
                send_sem=x_send.at[j, k],
                recv_sem=x_recv.at[j, k],
                device_id=at_x(k),
                device_id_type=MESH,
            )
            copy.start()
            copies.append(copy)
        pending.extend(copies)
        return copies

    def along_y(j, arriving):
        for copy in arriving:
            copy.wait_recv()
        copies = []
        for k in range(len(others)):
            target = at_y(k, 1)
            copy = pltpu.make_async_remote_copy(
                src_ref=relay.at[j, target[1]],
                dst_ref=out.at[j, t],
                send_sem=y_send.at[j, k],
                recv_sem=y_recv.at[j, k],
                device_id=target,
                device_id_type=MESH,
            )
            copy.start()
            copies.append(copy)
        pending.extend(copies)
        own = pltpu.make_async_copy(relay.at[j, t], out.at[j, t], own_sem.at[j])
        own.start()
        return copies, own

    pl.semaphore_wait(barrier, len(peers))
    arrivals = {}
    arrivals[1] = [along_z(0, 1, 1, 0, count, 1)]
    arrivals[7] = [along_z(0, 7, 7, 0, count, -1)]
    crossing = {}
    landing = []
    previous = None
    for j in ORDER:
        for copy in arrivals.get(j, ()):
            copy.wait_recv()
        if j in (1, 2):
            arrivals[j + 1] = [along_z(j, j + 1, j + 1, 0, count, 1)]
        if j in (7, 6):
            arrivals[j - 1] = [along_z(j, j - 1, j - 1, 0, count, -1)]
        if j == 3:
            arrivals[4] = [along_z(3, 4, 4, 0, FIRST_HALF, 1)]
        if j == 5:
            arrivals[4].append(along_z(5, 4, 0, FIRST_HALF, count - FIRST_HALF, -1))
        pick(j)
        crossing[j] = along_x(j)
        if previous is not None:
            landing.append(along_y(previous, crossing[previous]))
        previous = j
    landing.append(along_y(previous, crossing[previous]))
    for copies, own in landing:
        for copy in copies:
            copy.wait_recv()
        own.wait()
    for copy in pending:
        copy.wait_send()


def exchanged(requests, blocks):
    count = blocks.shape[0]
    block = blocks.shape[1:]
    gathered = [pltpu.VMEM((count, *block), blocks.dtype) for _ in range(NZ - 1)]
    return pl.pallas_call(
        exchange_kernel,
        out_shape=jax.ShapeDtypeStruct((NZ, NT, NX, *block), blocks.dtype),
        in_specs=[
            pl.BlockSpec(memory_space=pltpu.SMEM),
            pl.BlockSpec(memory_space=pltpu.VMEM),
        ],
        out_specs=pl.BlockSpec(memory_space=pl.ANY),
        scratch_shapes=gathered
        + [
            pltpu.VMEM((NZ, NX - 1, NT, *block), blocks.dtype),
            pltpu.VMEM((NZ, NT, NX, *block), blocks.dtype),
            pltpu.SemaphoreType.DMA((NZ,)),
            pltpu.SemaphoreType.DMA((NZ,)),
            pltpu.SemaphoreType.DMA((NZ, NX)),
            pltpu.SemaphoreType.DMA((NZ, NX)),
            pltpu.SemaphoreType.DMA((NZ, NT)),
            pltpu.SemaphoreType.DMA((NZ, NT)),
            pltpu.SemaphoreType.DMA((NZ,)),
        ],
        compiler_params=pltpu.CompilerParams(
            collective_id=1, has_side_effects=True, vmem_limit_bytes=40 * 2**20
        ),
    )(requests, blocks)


def three_parts(value):
    high = value.astype(jnp.bfloat16).astype(jnp.float32)
    rest = value - high
    middle = rest.astype(jnp.bfloat16).astype(jnp.float32)
    low = (rest - middle).astype(jnp.bfloat16).astype(jnp.float32)
    return high, middle, low


def pair_kernel(slots, used, held, out, left, right, inverse, spread, columns, product0, product1):
    row8 = lax.broadcasted_iota(jnp.int32, (8, BLK), 0)
    row = lax.broadcasted_iota(jnp.int32, (ROWS, BLK), 0)

    def prepare(slot, _):
        j, k = slot // NX, slot % NX
        chunk = [held[j, i, k].astype(jnp.float32) for i in range(NT)]
        zero = jnp.zeros((ROWS, BLK), jnp.float32)
        early = {i: jnp.where(row < HALF, chunk[i], zero) for i in (6, 7)}
        late = {i: jnp.where(row < HALF, zero, chunk[i]) for i in (0, 1)}
        kept = [
            [chunk[0], chunk[1]] + chunk[2:6] + [early[6], zero],
            [late[0], chunk[1]] + chunk[2:6] + [chunk[6], zero],
            [zero, chunk[1]] + chunk[2:6] + [chunk[6], early[7]],
            [zero, late[1]] + chunk[2:6] + [chunk[6], chunk[7]],
        ]

        def folded(a):
            return jnp.sum(a.reshape(ROWS // 8, 8, BLK), axis=0)

        def both(a):
            return folded(a), folded(a * a)

        middle = [folded(chunk[2] + chunk[3] + chunk[4] + chunk[5])]
        middle.append(folded(sum(chunk[i] * chunk[i] for i in range(2, 6))))
        ends = {}
        sums, weights = [], []
        for w in range(NW):
            first, second = middle
            for i in (0, 1, 6, 7):
                part = kept[w][i]
                if part is zero:
                    continue
                if id(part) not in ends:
                    ends[id(part)] = both(part)
                first = first + ends[id(part)][0]
                second = second + ends[id(part)][1]
            first = jnp.sum(first, axis=0, keepdims=True)
            second = jnp.sum(second, axis=0, keepdims=True)
            center = first / WIN
            variance = second / WIN - center * center
            sums.append(first)
            weights.append(1.0 / (variance + epsilon))
        inverse[slot] = jnp.concatenate(weights + weights, axis=0)
        for w in range(NW):
            spread[slot, w] = jnp.transpose(jnp.broadcast_to(weights[w], (BLK, BLK)))

        def with_rows(tail, values):
            for n, value in enumerate(values):
                tail = jnp.where(row8 == 4 + n, jnp.broadcast_to(value, (8, BLK)), tail)
            return tail

        edge = ROWS - 8
        whole = list(chunk)
        for w in range(NW):
            h, m, l = three_parts(-sums[w])
            lefts = [h, h, m, h, l, m, m, l]
            h, m, l = three_parts(sums[w] / WIN)
            rights = [h, m, h, l, h, m, l, m]
            for n in range(2):
                i = 2 * w + n
                part = slice(4 * n, 4 * n + 4)
                whole[i] = jnp.concatenate(
                    [whole[i][:edge], with_rows(whole[i][edge:], lefts[part])], axis=0
                )
                kept[w][i] = jnp.concatenate(
                    [kept[w][i][:edge], with_rows(kept[w][i][edge:], rights[part])], axis=0
                )
            for i in range(NT):
                right[slot, pl.ds(i * ROWS, ROWS), pl.ds(w * BLK, BLK)] = kept[w][i].astype(
                    jnp.bfloat16
                )
        for i in range(0, NT, 2):
            two = jnp.concatenate([whole[i], whole[i + 1]], axis=0)
            left[slot, :, pl.ds(i * ROWS, 2 * ROWS)] = jnp.transpose(two).astype(jnp.bfloat16)
        return 0

    lax.fori_loop(0, NA, prepare, 0)

    pairs = out.shape[0]
    group = BLK // NW
    lane = lax.broadcasted_iota(jnp.int32, (BLK, BLK), 1)
    scale = 1.0 / (WIN * BLK)

    def multiply(p, product):
        a, b = slots[p, 0], slots[p, 1]
        product[...] = jnp.dot(left[a], right[b], preferred_element_type=jnp.float32)

    def reduce(p, product):
        a, b = slots[p, 0], slots[p, 1]
        within = lax.rem(p, group) * NW
        keep = columns[...]
        rows = []
        for w in range(NW):
            value = product[:, pl.ds(w * BLK, BLK)]
            scaled = value * value * spread[a, w]
            weight = inverse[b, pl.ds(w, 1)]
            over_j = jnp.sum(scaled * weight, axis=1, keepdims=True) * scale
            over_i = jnp.sum(scaled, axis=0, keepdims=True) * (weight * scale)
            keep = jnp.where(lane == within + w, over_j, keep)
            rows.append(jnp.where(p < used[0], over_i, 0.0))
        columns[...] = keep
        out[p] = jnp.concatenate([r for over_i in rows for r in (over_i, over_i)], axis=0)

    def block(n, _):
        columns[...] = jnp.zeros_like(columns)

        def two(m, _):
            p = n * group + 2 * m
            multiply(p + 1, product1)
            reduce(p, product0)
            multiply(jnp.minimum(p + 2, pairs - 1), product0)
            reduce(p + 1, product1)
            return 0

        lax.fori_loop(0, group // 2, two, 0)
        turned = jnp.transpose(columns[...])
        number = lax.broadcasted_iota(jnp.int32, (BLK, BLK), 0) // NW + n * group
        turned = jnp.where(number < used[0], turned, 0.0).reshape(group, NW, BLK)
        for w in range(NW):
            out[pl.ds(n * group, group), 2 * w, :] = turned[:, w, :]
        return 0

    multiply(0, product0)
    lax.fori_loop(0, pairs // group, block, 0)


def correlated(slots, used, held):
    pairs = slots.shape[0]
    minutes = NT * ROWS
    return pl.pallas_call(
        pair_kernel,
        out_shape=jax.ShapeDtypeStruct((pairs, 2 * NW, BLK), jnp.float32),
        in_specs=[
            pl.BlockSpec(memory_space=pltpu.SMEM),
            pl.BlockSpec(memory_space=pltpu.SMEM),
            pl.BlockSpec(memory_space=pltpu.VMEM),
        ],
        out_specs=pl.BlockSpec(memory_space=pltpu.VMEM),
        scratch_shapes=[
            pltpu.VMEM((NA, BLK, minutes), jnp.bfloat16),
            pltpu.VMEM((NA, minutes, NW * BLK), jnp.bfloat16),
            pltpu.VMEM((NA, 8, BLK), jnp.float32),
            pltpu.VMEM((NA, NW, BLK, BLK), jnp.float32),
            pltpu.VMEM((BLK, BLK), jnp.float32),
            pltpu.VMEM((BLK, NW * BLK), jnp.float32),
            pltpu.VMEM((BLK, NW * BLK), jnp.float32),
        ],
        compiler_params=pltpu.CompilerParams(vmem_limit_bytes=56 * 2**20),
    )(slots, used, held)


def on_device(prices, sectors, wanted, pair_slots, pair_count):
    stretch = prices.shape[0]
    column_index = lax.axis_index("asset")
    stretch_index = lax.axis_index("tm")
    x, z = column_index // NZ, column_index % NZ
    previous = shifted(prices[stretch - 1 :], "tm", 1)
    earlier = jnp.concatenate([previous, prices[: stretch - 1]], axis=0)
    minute = stretch_index * stretch + lax.iota(jnp.int32, stretch)
    returns = jnp.where((minute > 0)[:, None], prices - earlier, jnp.zeros((), jnp.float32))
    labels = lax.iota(jnp.int32, SECT)
    member = (sectors[:, None] == labels[None, :]).astype(jnp.float32)
    totals = jnp.dot(returns, member, precision=highest)
    members = jnp.sum(member, axis=0)
    message = jnp.concatenate([totals.ravel(), members])
    message = jnp.pad(message, (0, 8 * BLK - message.size)).reshape(8, BLK)
    message = summed(message).ravel()
    totals = message[: stretch * SECT].reshape(stretch, SECT)
    members = message[stretch * SECT : (stretch + 1) * SECT]
    sector_mean = totals / members
    neutral = (returns - jnp.dot(sector_mean, member.T, precision=highest)).astype(jnp.bfloat16)
    count = prices.shape[1] // BLK
    neutral = jnp.pad(neutral, ((0, ROWS - stretch), (0, 0)))
    blocks = jnp.transpose(neutral.reshape(ROWS, count, BLK), (1, 0, 2))

    table = wanted.reshape(NX, NZ, NT, NX, NZ)
    table = lax.dynamic_index_in_dim(table, z, 1, keepdims=False)
    table = lax.dynamic_index_in_dim(table, x, 2, keepdims=False)
    from_z = (z - lax.iota(jnp.int32, NZ)) % NZ
    to_x = (x + lax.iota(jnp.int32, NX)) % NX
    table = jnp.take(jnp.take(table, to_x, axis=0), from_z, axis=2)
    requests = jnp.maximum(jnp.transpose(table, (2, 0, 1)).ravel(), 0)
    held = exchanged(requests, blocks)

    slots = ((z - pair_slots % NZ) % NZ) * NX + (x - pair_slots // NZ) % NX
    summary = correlated(slots, pair_count, held)
    return summary.reshape(summary.shape[0], NW, 2, BLK)


def solution(mesh):
    placed = (P("tm", "asset"), P("asset"), P(), P(("asset", "tm"), None), P(("asset", "tm")))
    return jax.shard_map(
        on_device,
        mesh=mesh,
        in_specs=placed,
        out_specs=P(("asset", "tm"), None, None, None),
        check_vma=False,
    )
```

```python
import functools

import jax
import jax.numpy as jnp
from jax import lax
from jax.experimental import pallas as pl
from jax.experimental.pallas import tpu as pltpu
from jax.sharding import PartitionSpec as P

BLK = 128
NX, NZ, NY, NC = 4, 8, 4, 2
NA, NT = NX * NZ, NY * NC
ROWS = 64
MINUTES = 60
HALF = 30
WIN = 390
NW = 4
MESH = pl.DeviceIdType.MESH

epsilon = 1e-06


def shifted(block, axis, distance):
    devices = range(lax.axis_size(axis))
    route = [(i - distance, i) for i in devices if i - distance in devices]
    return lax.ppermute(block, axis, route)


def three_parts(value):
    high = value.astype(jnp.bfloat16).astype(jnp.float32)
    rest = value - high
    middle = rest.astype(jnp.bfloat16).astype(jnp.float32)
    low = (rest - middle).astype(jnp.bfloat16).astype(jnp.float32)
    return high, middle, low


def front_kernel(
    prices, previous, sectors, blocks, mine, line, from_x, from_z, x_send, x_recv, z_send, z_recv
):
    d = lax.axis_index("asset")
    t = lax.axis_index("tm")
    x, z = d // NZ, d % NZ
    x_peers = [((x + k) % NX) * NZ + z for k in range(1, NX)]
    z_peers = [x * NZ + (z + k) % NZ for k in range(1, NZ)]
    barrier = pltpu.get_barrier_semaphore()
    for peer in x_peers + z_peers:
        pl.semaphore_signal(barrier, inc=1, device_id=(peer, t), device_id_type=MESH)

    width = prices.shape[1]
    labels = 16
    price = prices[...]
    earlier = jnp.concatenate([previous[...], price[: MINUTES - 1]], axis=0)
    row = lax.broadcasted_iota(jnp.int32, (MINUTES, width), 0)
    returns = jnp.where((row == 0) & (t == 0), 0.0, price - earlier)
    spare = lax.broadcasted_iota(jnp.int32, (ROWS - MINUTES, width), 0)
    ones = jnp.where(spare == 0, 1.0, 0.0)
    parts = three_parts(jnp.concatenate([returns, ones], axis=0))
    label = lax.broadcasted_iota(jnp.int32, (labels, width), 0)
    member = jnp.where(label == sectors[...], 1.0, 0.0).astype(jnp.bfloat16)
    totals = jnp.zeros((labels, ROWS), jnp.float32)
    for part in parts:
        totals = totals + lax.dot_general(
            member,
            part.astype(jnp.bfloat16),
            (((1,), (1,)), ((), ())),
            preferred_element_type=jnp.float32,
        )
    mine[...] = jnp.concatenate([totals[:8], totals[8:]], axis=1)
    pl.semaphore_wait(barrier, len(x_peers) + len(z_peers))

    def gather(source, slots, peers, send_sem, recv_sem):
        copies = []
        for k, peer in enumerate(peers):
            copy = pltpu.make_async_remote_copy(
                src_ref=source,
                dst_ref=slots.at[k],
                send_sem=send_sem.at[k],
                recv_sem=recv_sem.at[k],
                device_id=(peer, t),
                device_id_type=MESH,
            )
            copy.start()
            copies.append(copy)
        for copy in copies:
            copy.wait_recv()
        total = source[...]
        for k in range(len(peers)):
            total = total + slots[k]
        return total, copies

    total, sent = gather(mine, from_x, x_peers, x_send, x_recv)
    line[...] = total
    total, more = gather(line, from_z, z_peers, z_send, z_recv)
    totals = jnp.concatenate([total[:, :ROWS], total[:, ROWS:]], axis=0)
    members = totals[:, MINUTES : MINUTES + 1]
    mean = totals / jnp.where(members > 0, members, 1.0)
    parts = jnp.concatenate(three_parts(mean), axis=0)
    parts = jnp.concatenate([parts, jnp.zeros((BLK - 3 * labels, ROWS), jnp.float32)], axis=0)
    parts = jnp.concatenate([parts, jnp.zeros((BLK, BLK - ROWS), jnp.float32)], axis=1)
    by_minute = jnp.transpose(parts)[:ROWS, : 3 * labels].astype(jnp.bfloat16)
    members3 = jnp.concatenate([member, member, member], axis=0)
    common = jnp.dot(by_minute, members3, preferred_element_type=jnp.float32)
    neutral = jnp.concatenate([returns, ones], axis=0) - common
    for n in range(width // BLK):
        blocks[n] = neutral[:, n * BLK : (n + 1) * BLK].astype(jnp.bfloat16)
    for copy in sent + more:
        copy.wait_send()


def neutral_blocks(prices, previous, sectors):
    return pl.pallas_call(
        front_kernel,
        out_shape=jax.ShapeDtypeStruct((prices.shape[1] // BLK, ROWS, BLK), jnp.bfloat16),
        in_specs=[pl.BlockSpec(memory_space=pltpu.VMEM)] * 3,
        out_specs=pl.BlockSpec(memory_space=pltpu.VMEM),
        scratch_shapes=[
            pltpu.VMEM((8, BLK), jnp.float32),
            pltpu.VMEM((8, BLK), jnp.float32),
            pltpu.VMEM((NX - 1, 8, BLK), jnp.float32),
            pltpu.VMEM((NZ - 1, 8, BLK), jnp.float32),
            pltpu.SemaphoreType.DMA((NX - 1,)),
            pltpu.SemaphoreType.DMA((NX - 1,)),
            pltpu.SemaphoreType.DMA((NZ - 1,)),
            pltpu.SemaphoreType.DMA((NZ - 1,)),
        ],
        compiler_params=pltpu.CompilerParams(collective_id=0, has_side_effects=True),
    )(prices, previous, sectors)


ORDER = (0, 1, 7, 2, 6, 3, 5, 4)
FIRST_HALF = 8
PLACE = (0, 1, 3, 2)


def exchange_kernel(
    requests, blocks, out, g1, g2, g3, g4, g5, g6, g7, picked, relay,
    z_send, z_recv, x_send, x_recv, y_send, y_recv, own_sem,
):
    d = lax.axis_index("asset")
    t = lax.axis_index("tm")
    x, z, y, c = d // NZ, d % NZ, t // NC, t % NC
    gathered = (blocks, g1, g2, g3, g4, g5, g6, g7)
    count = blocks.shape[0]
    minutes = pl.ds(0, MINUTES)

    def at_x(k):
        return ((x + k) % NX) * NZ + z, t

    def at_z(k):
        return x * NZ + (z + k + NZ) % NZ, t

    others = [(dy, dc) for dy in (1, 3, 2, 0) for dc in (0, 1) if (dy, dc) != (0, 0)]

    def at_y(k, sign):
        dy, dc = others[k]
        return d, ((y + sign * dy + NY) % NY) * NC + (c + dc) % NC

    barrier = pltpu.get_barrier_semaphore()
    peers = [at_z(1), at_z(-1)] + [at_x(k) for k in range(1, NX)]
    peers += [at_y(k, 1) for k in range(len(others))]
    for peer in peers:
        pl.semaphore_signal(barrier, inc=1, device_id=peer, device_id_type=MESH)

    pending = []

    def along_z(source, target, number, first, size, step):
        copy = pltpu.make_async_remote_copy(
            src_ref=gathered[source].at[pl.ds(first, size), minutes],
            dst_ref=gathered[target].at[pl.ds(first, size), minutes],
            send_sem=z_send.at[number],
            recv_sem=z_recv.at[number],
            device_id=at_z(step),
            device_id_type=MESH,
        )
        copy.start()
        pending.append(copy)
        return copy

    def pick(j):
        column = x * NZ + (z + NZ - j) % NZ
        for k in (1, 3, 2, 0):
            def one(i, _):
                block = gathered[j][jnp.maximum(requests[(x + k) % NX, i, column], 0)]
                if k == 0:
                    relay[j, i, PLACE[0]] = block
                else:
                    picked[j, k - 1, i] = block
                return 0
            lax.fori_loop(0, NT, one, 0)

    def along_x(j):
        copies = []
        for k in (1, 3, 2):
            copy = pltpu.make_async_remote_copy(
                src_ref=picked.at[j, k - 1, :, minutes],
                dst_ref=relay.at[j, :, PLACE[k], minutes],
                send_sem=x_send.at[j, k],
                recv_sem=x_recv.at[j, k],
                device_id=at_x(k),
                device_id_type=MESH,
            )
            copy.start()
            copies.append(copy)
        pending.extend(copies)
        return copies

    def along_y(j, arriving):
        copies = []
        for part, (first, size) in enumerate(((0, NX - 1), (NX - 1, 1))):
            for copy in arriving[:2] if part == 0 else arriving[2:]:
                copy.wait_recv()
            places = pl.ds(first, size)
            for k in range(len(others)):
                target = at_y(k, 1)
                copy = pltpu.make_async_remote_copy(
                    src_ref=relay.at[j, target[1], places, minutes],
                    dst_ref=out.at[j, t, places, minutes],
                    send_sem=y_send.at[j, part, k],
                    recv_sem=y_recv.at[j, part, k],
                    device_id=target,
                    device_id_type=MESH,
                )
                copy.start()
                copies.append(copy)
        pending.extend(copies)
        own = pltpu.make_async_copy(relay.at[j, t], out.at[j, t], own_sem.at[j])
        own.start()
        return copies, own

    pick(ORDER[0])
    pl.semaphore_wait(barrier, len(peers))
    arrivals = {}
    arrivals[1] = [along_z(0, 1, 1, 0, count, 1)]
    arrivals[7] = [along_z(0, 7, 7, 0, count, -1)]
    crossing = {}
    landing = []
    previous = None
    for j in ORDER:
        for copy in arrivals.get(j, ()):
            copy.wait_recv()
        if j in (1, 2):
            arrivals[j + 1] = [along_z(j, j + 1, j + 1, 0, count, 1)]
        if j in (7, 6):
            arrivals[j - 1] = [along_z(j, j - 1, j - 1, 0, count, -1)]
        if j == 3:
            arrivals[4] = [along_z(3, 4, 4, 0, FIRST_HALF, 1)]
        if j == 5:
            arrivals[4].append(along_z(5, 4, 0, FIRST_HALF, count - FIRST_HALF, -1))
        if j != ORDER[0]:
            pick(j)
        crossing[j] = along_x(j)
        if previous is not None:
            landing.append(along_y(previous, crossing[previous]))
        previous = j
    landing.append(along_y(previous, crossing[previous]))
    for copies, own in landing:
        for copy in copies:
            copy.wait_recv()
        own.wait()
    for copy in pending:
        copy.wait_send()


def exchanged(requests, blocks):
    count = blocks.shape[0]
    block = blocks.shape[1:]
    gathered = [pltpu.VMEM((count, *block), blocks.dtype) for _ in range(NZ - 1)]
    return pl.pallas_call(
        exchange_kernel,
        out_shape=jax.ShapeDtypeStruct((NZ, NT, NX, *block), blocks.dtype),
        in_specs=[
            pl.BlockSpec(memory_space=pltpu.SMEM),
            pl.BlockSpec(memory_space=pltpu.VMEM),
        ],
        out_specs=pl.BlockSpec(memory_space=pl.ANY),
        scratch_shapes=gathered
        + [
            pltpu.VMEM((NZ, NX - 1, NT, *block), blocks.dtype),
            pltpu.VMEM((NZ, NT, NX, *block), blocks.dtype),
            pltpu.SemaphoreType.DMA((NZ,)),
            pltpu.SemaphoreType.DMA((NZ,)),
            pltpu.SemaphoreType.DMA((NZ, NX)),
            pltpu.SemaphoreType.DMA((NZ, NX)),
            pltpu.SemaphoreType.DMA((NZ, 2, NT)),
            pltpu.SemaphoreType.DMA((NZ, 2, NT)),
            pltpu.SemaphoreType.DMA((NZ,)),
        ],
        compiler_params=pltpu.CompilerParams(
            collective_id=1, has_side_effects=True, vmem_limit_bytes=40 * 2**20
        ),
    )(requests, blocks)


def pair_kernel(
    slots, used, held, out, near, left, right, inverse, spread, columns, product0, product1, sem
):
    loads = [pltpu.make_async_copy(held.at[j], near.at[j], sem.at[j]) for j in range(NZ)]
    for load in loads:
        load.start()
    tile = 16
    row = lax.broadcasted_iota(jnp.int32, (tile, BLK), 0)
    zero = jnp.zeros((tile, BLK), jnp.float32)
    tiles = ROWS // tile
    spare = MINUTES - (tiles - 1) * tile

    def folded(parts):
        total = parts[0]
        for part in parts[1:]:
            total = total + part
        return total[:8] + total[8:]

    def both(parts):
        return folded(parts), folded([part * part for part in parts])

    def with_rows(tail, values):
        for n, value in enumerate(values):
            tail = jnp.where(row == spare + n, jnp.broadcast_to(value, (tile, BLK)), tail)
        return tail

    def prepare(j, k):
        slot = j * NX + k
        packed, wide = [], []
        for i in range(NT):
            whole = near[j, i, k]
            packed.append([whole[tile * q : tile * q + tile] for q in range(tiles)])
            wide.append([part.astype(jnp.float32) for part in packed[i]])
            wide[i][-1] = jnp.where(row < spare, wide[i][-1], zero)
            packed[i][-1] = wide[i][-1].astype(jnp.bfloat16)
        blank = zero.astype(jnp.bfloat16)
        cut = HALF - tile
        halves = {}
        for i in (0, 1, 6, 7):
            early = jnp.where(row < cut, wide[i][1], zero)
            late = jnp.where(row < cut, zero, wide[i][1])
            halves[i, 0] = both([wide[i][0], early])
            halves[i, 1] = both([late] + wide[i][2:])
            if i < 2:
                packed.append([blank, late.astype(jnp.bfloat16)] + packed[i][2:])
            else:
                packed.append([packed[i][0], early.astype(jnp.bfloat16), blank, blank])
        late0, late1, early6, early7 = packed[NT:]
        none = [blank] * tiles
        kept = [
            [packed[0], packed[1]] + packed[2:6] + [early6, none],
            [late0, packed[1]] + packed[2:6] + [packed[6], none],
            [none, packed[1]] + packed[2:6] + [packed[6], early7],
            [none, late1] + packed[2:6] + [packed[6], packed[7]],
        ]
        middle = both([part for i in range(2, 6) for part in wide[i]])
        inside = [middle[n] + halves[1, 1][n] + halves[6, 0][n] for n in range(2)]
        extra = (
            ((0, 0), (0, 1), (1, 0)),
            ((0, 1), (1, 0), (6, 1)),
            ((1, 0), (6, 1), (7, 0)),
            ((6, 1), (7, 0), (7, 1)),
        )
        weights, lefts, rights = [], [], []
        for w in range(NW):
            first, second = inside
            for part in extra[w]:
                first = first + halves[part][0]
                second = second + halves[part][1]
            first = jnp.sum(first, axis=0, keepdims=True)
            second = jnp.sum(second, axis=0, keepdims=True)
            center = first / WIN
            variance = second / WIN - center * center
            weights.append(1.0 / (variance + epsilon))
            h, m, l = three_parts(-first)
            lefts += [h, h, m, h, l, m, m, l]
            h, m, l = three_parts(center)
            rights += [h, m, h, l, h, m, l, m]
        inverse[slot] = jnp.concatenate(weights + weights, axis=0)
        for w in range(NW):
            spread[slot, w] = jnp.transpose(jnp.broadcast_to(weights[w], (BLK, BLK)))
        rest = ROWS - MINUTES
        for w in range(NW):
            for i in range(NT):
                parts = list(kept[w][i])
                if i // 2 == w:
                    tail = parts[-1].astype(jnp.float32)
                    parts[-1] = with_rows(tail, rights[rest * i : rest * i + rest]).astype(jnp.bfloat16)
                for q in range(tiles):
                    right[slot, pl.ds(i * ROWS + tile * q, tile), pl.ds(w * BLK, BLK)] = parts[q]
        for i in range(0, NT, 2):
            parts = []
            for n in (i, i + 1):
                tail = with_rows(wide[n][-1], lefts[rest * n : rest * n + rest])
                parts += wide[n][:-1] + [tail]
            left[slot, :, pl.ds(i * ROWS, 2 * ROWS)] = jnp.transpose(jnp.concatenate(parts, axis=0)).astype(jnp.bfloat16)
        return j

    def arrive(j, _):
        pltpu.make_async_copy(held.at[j], near.at[j], sem.at[j]).wait()
        for k in range(NX):
            prepare(j, k)
        return 0

    lax.fori_loop(0, NZ, arrive, 0)

    pairs = out.shape[0]
    products = (product0, product1)
    group = BLK // NW
    lane8 = lax.broadcasted_iota(jnp.int32, (8, BLK), 1)
    scale = 1.0 / (WIN * BLK)

    def multiply(p, product, half):
        a, b = slots[0, p], slots[1, p]
        part = pl.ds(2 * half * BLK, 2 * BLK)
        product[:, part] = jnp.dot(left[a], right[b, :, part], preferred_element_type=jnp.float32)

    def reduce(p, product, half):
        a, b = slots[0, p], slots[1, p]
        within = lax.rem(p, group) * NW
        windows = (2 * half, 2 * half + 1)
        weight = {w: inverse[b, pl.ds(w, 1)] for w in windows}
        total = {w: jnp.zeros((8, BLK), jnp.float32) for w in windows}
        for i in range(BLK // 8):
            rows = pl.ds(8 * i, 8)
            keep = columns[rows, :]
            for w in windows:
                value = product[rows, pl.ds(w * BLK, BLK)]
                scaled = value * value * spread[a, w, rows]
                total[w] = total[w] + scaled
                over_j = jnp.sum(scaled * weight[w], axis=1, keepdims=True)
                keep = jnp.where(lane8 == within + w, over_j, keep)
            columns[rows, :] = keep
        for w in windows:
            over_i = jnp.sum(total[w], axis=0, keepdims=True) * (weight[w] * scale)
            out[p, pl.ds(2 * w + 1, 1)] = jnp.where(p < used[0], over_i, 0.0)

    def block(n, _):
        def several(m, _):
            p = n * group + 8 * m
            for u in range(8):
                after = p + u + 1 if u < 7 else jnp.minimum(p + 8, pairs - 1)
                for half in range(2):
                    multiply(after, products[1 - u % 2], half)
                    reduce(p + u, products[u % 2], half)
            return 0

        lax.fori_loop(0, group // 8, several, 0)
        turned = jnp.transpose(columns[...]) * scale
        number = lax.broadcasted_iota(jnp.int32, (BLK, BLK), 0) // NW + n * group
        turned = jnp.where(number < used[0], turned, 0.0).reshape(group, NW, BLK)
        for w in range(NW):
            out[pl.ds(n * group, group), 2 * w, :] = turned[:, w, :]
        return 0

    columns[...] = jnp.zeros_like(columns)
    for half in range(2):
        multiply(0, product0, half)
    lax.fori_loop(0, pairs // group, block, 0)


def correlated(slots, used, held):
    pairs = slots.shape[1]
    minutes = NT * ROWS
    return pl.pallas_call(
        pair_kernel,
        out_shape=jax.ShapeDtypeStruct((pairs, 2 * NW, BLK), jnp.float32),
        in_specs=[
            pl.BlockSpec(memory_space=pltpu.SMEM),
            pl.BlockSpec(memory_space=pltpu.SMEM),
            pl.BlockSpec(memory_space=pltpu.HBM),
        ],
        out_specs=pl.BlockSpec(memory_space=pltpu.VMEM),
        scratch_shapes=[
            pltpu.VMEM(held.shape, held.dtype),
            pltpu.VMEM((NA, BLK, minutes), jnp.bfloat16),
            pltpu.VMEM((NA, minutes, NW * BLK), jnp.bfloat16),
            pltpu.VMEM((NA, 8, BLK), jnp.float32),
            pltpu.VMEM((NA, NW, BLK, BLK), jnp.float32),
            pltpu.VMEM((BLK, BLK), jnp.float32),
            pltpu.VMEM((BLK, NW * BLK), jnp.float32),
            pltpu.VMEM((BLK, NW * BLK), jnp.float32),
            pltpu.SemaphoreType.DMA((NZ,)),
        ],
        compiler_params=pltpu.CompilerParams(vmem_limit_bytes=56 * 2**20),
    )(slots, used, held)


def on_device(prices, sectors, wanted, pair_slots, pair_count):
    stretch = prices.shape[0]
    column_index = lax.axis_index("asset")
    x, z = column_index // NZ, column_index % NZ
    previous = shifted(prices[stretch - 1 :], "tm", 1)
    blocks = neutral_blocks(prices, previous, sectors.reshape(1, -1))

    requests = lax.dynamic_index_in_dim(wanted.reshape(NX, NZ, NT, NA), z, 1, keepdims=False)
    held = exchanged(requests, blocks)

    across = (x - pair_slots // NZ) % NX
    across = jnp.where(across > 1, 5 - across, across)
    slots = (((z - pair_slots) % NZ) * NX + across).T
    summary = correlated(slots, pair_count, held)
    return summary.reshape(summary.shape[0], NW, 2, BLK)


def solution(mesh):
    placed = (P("tm", "asset"), P("asset"), P(), P(("asset", "tm"), None), P(("asset", "tm")))
    return jax.shard_map(
        on_device,
        mesh=mesh,
        in_specs=placed,
        out_specs=P(("asset", "tm"), None, None, None),
        check_vma=False,
    )
```
